256 devices in a mesh: wide: 32 (over x, y, z_hi), narrow: 8 (over z_lo, core).
Axes of the slice: x: 4, y: 4, z: 8 (z_hi: 2, z_lo: 4; z = z_hi * 4 + z_lo), core: 2. Of those that a mesh axis runs over, the one named last changes fastest.
Arguments:
- amplitudes: float32 [262144, 128], P(('wide', 'narrow')), may hold values from -6 to 6
- top_gates: float32 [4, 2, 32, 32], replicated, may hold values from -0.32 to 1.21
- mid_gates: float32 [3, 2, 32, 32], replicated, may hold values from -0.32 to 1.21
- low_gates: float32 [3, 2, 64, 64], replicated, may hold values from -0.32 to 1.21
- ham_top: float32 [3, 2, 2, 32, 32], replicated, may hold values from -0.32 to 1.21
- ham_mid: float32 [3, 2, 32, 32], replicated, may hold values from -0.32 to 1.21
- ham_low: float32 [3, 2, 64, 64], replicated, may hold values from -0.32 to 1.21
- flip_masks: int32 [3], replicated, may hold values from 0 to 65535
- phase_masks: int32 [3], replicated, may hold values from 0 to 65535
- device_phase_masks: int32 [3], replicated, may hold values from 0 to 255
Outputs:
- final_state: float32 [262144, 128], P(('wide', 'narrow'))
- cotangent: float32 [262144, 128], P(('wide', 'narrow'))
The draws below stay inside these ranges and needn't reach their ends.
All inputs are finite; a program needn't handle non-finite values.
Results may differ from the reference program's by a relative error of at most 0.00014.
Values sent between devices are 32-bit elements; how exact they have to be, the bound alone decides.
No kernel may reach another device: no remote copies, remote signals or barrier semaphores. Data moves between devices by JAX's collectives and lax.ppermute only.
A program may use at most 64 MiB of HBM per device.

```python
import math
from functools import partial
import jax
import jax.numpy as jnp
from jax import lax

TOP = 32
MID = 32
LOW = 64
ROUNDS = 3
BLOCKS = 3
ROWS = 262144
GLOBAL_STATES = 256
N_WIDE = 32
N_NARROW = 8


def draw_operator(key, count, order):
    key_re, key_im = jax.random.split(key)
    noise_re = jnp.clip(jax.random.normal(key_re, (count, order, order), jnp.float32), -4.0, 4.0)
    noise_im = jnp.clip(jax.random.normal(key_im, (count, order, order), jnp.float32), -4.0, 4.0)
    spread = 0.35 / math.sqrt(order)
    norm_factor = math.sqrt(1.0 + 2.0 * 0.35 * 0.35)
    identity = jnp.eye(order, dtype=jnp.float32)
    real_part = (identity[None] + spread * noise_re) / norm_factor
    imag_part = spread * noise_im / norm_factor
    return jnp.stack([real_part, imag_part], axis=1)


def draw_top_gates(key, part):
    return draw_operator(jax.random.fold_in(key, 11), ROUNDS + 1, TOP)


def draw_mid_gates(key, part):
    return draw_operator(jax.random.fold_in(key, 12), ROUNDS, MID)


def draw_low_gates(key, part):
    return draw_operator(jax.random.fold_in(key, 13), ROUNDS, LOW)


def draw_ham_top(key, part):
    stacked = draw_operator(jax.random.fold_in(key, 14), BLOCKS * 2, TOP)
    return stacked.reshape(BLOCKS, 2, 2, TOP, TOP)


def draw_ham_mid(key, part):
    return draw_operator(jax.random.fold_in(key, 15), BLOCKS, MID)


def draw_ham_low(key, part):
    return draw_operator(jax.random.fold_in(key, 16), BLOCKS, LOW)


def level_of(stream_key, dims, cuts, low, high):
    level, own = 1.0, jax.random.fold_in(stream_key, 6)
    for dim, parts in cuts:
        heights = jnp.exp(jax.random.uniform(jax.random.fold_in(own, dim), (parts,), jnp.float32, low / len(cuts), high / len(cuts)))
        level = level * jnp.repeat(heights, dims[dim] // parts).reshape([-1 if axis == dim else 1 for axis in range(len(dims))])
    return level


def centred(stream_key, dims, scale, bound, shards=(), kind=jnp.bfloat16):
    level = level_of(stream_key, dims, shards, -0.22, 0.18) if shards else 1.0
    values = jax.random.normal(stream_key, dims, jnp.float32) * scale * level
    return jnp.minimum(jnp.maximum(values, -bound), bound).astype(kind)


def setup_inputs(seed: int = 0) -> dict:
    streams_of = jax.random.split(jax.random.key(seed), 11)
    amplitudes = centred(streams_of[0], (ROWS, 2 * LOW), 1.0, 6.0, ((0, 256),), jnp.float32)
    top_gates = draw_top_gates(jax.random.fold_in(streams_of[10], 71), 0)
    mid_gates = draw_mid_gates(jax.random.fold_in(streams_of[10], 71), 0)
    low_gates = draw_low_gates(jax.random.fold_in(streams_of[10], 71), 0)
    ham_top = draw_ham_top(jax.random.fold_in(streams_of[10], 71), 0)
    ham_mid = draw_ham_mid(jax.random.fold_in(streams_of[10], 71), 0)
    ham_low = draw_ham_low(jax.random.fold_in(streams_of[10], 71), 0)
    flip_masks = jax.random.randint(streams_of[7], (BLOCKS,), 0, TOP * MID * LOW).astype(jnp.int32)
    phase_masks = jax.random.randint(streams_of[8], (BLOCKS,), 0, TOP * MID * LOW).astype(jnp.int32)
    device_phase_masks = jax.random.randint(streams_of[9], (BLOCKS,), 0, GLOBAL_STATES).astype(jnp.int32)
    return dict(amplitudes=amplitudes, top_gates=top_gates, mid_gates=mid_gates, low_gates=low_gates, ham_top=ham_top, ham_mid=ham_mid, ham_low=ham_low, flip_masks=flip_masks, phase_masks=phase_masks, device_phase_masks=device_phase_masks)


HIGH = lax.Precision.HIGHEST


def product(pattern, mat_re, mat_im, field_re, field_im):
    contract = partial(jnp.einsum, pattern, precision=HIGH)
    return (contract(mat_re, field_re) - contract(mat_im, field_im),
            contract(mat_re, field_im) + contract(mat_im, field_re))


def parity(values, selector):
    folded = jnp.bitwise_and(values, selector)
    for offset in (16, 8, 4, 2, 1):
        folded = jnp.bitwise_xor(folded, jnp.right_shift(folded, offset))
    odd_bit = jnp.bitwise_and(folded, 1)
    return (1 - 2 * odd_bit).astype(jnp.float32)


def act_top(fields, matrix):
    blocks = matrix.reshape(2, N_WIDE, TOP // N_WIDE, N_WIDE, TOP // N_WIDE)
    return product('pqrs,rnasbc->pnaqbc', blocks[0], blocks[1], fields[0], fields[1])


def act_high(fields, matrix):
    blocks = matrix.reshape(2, N_WIDE, TOP // N_WIDE, N_WIDE, TOP // N_WIDE)
    return product('pqrs,wnrsbc->wnpqbc', blocks[0], blocks[1], fields[0], fields[1])


def act_mid(fields, matrix):
    return product('ij,wnasjc->wnasic', matrix[0], matrix[1], fields[0], fields[1])


def act_low(fields, matrix):
    return product('ij,wnasbj->wnasbi', matrix[0], matrix[1], fields[0], fields[1])


def layout(fields):
    return jnp.concatenate([fields[0].reshape(-1, LOW), fields[1].reshape(-1, LOW)], axis=1)


def reference(amplitudes, top_gates, mid_gates, low_gates, ham_top, ham_mid, ham_low, flip_masks, phase_masks, device_phase_masks):
    shape = (N_WIDE, N_NARROW, N_WIDE, TOP // N_WIDE, MID, LOW)
    fields = (amplitudes[:, :LOW].reshape(shape), amplitudes[:, LOW:].reshape(shape))
    for round_id in range(ROUNDS):
        fields = act_top(fields, top_gates[round_id])
        fields = act_mid(fields, mid_gates[round_id])
        fields = act_low(fields, low_gates[round_id])
    fields = act_top(fields, top_gates[ROUNDS])
    final_state = layout(fields)
    split = (N_WIDE, N_NARROW, TOP, MID, LOW)
    devices = jnp.arange(N_WIDE * N_NARROW, dtype=jnp.int32).reshape(N_WIDE, N_NARROW)
    flips_wide = (True, False, True)
    flips_narrow = (False, True, True)
    total_re = jnp.zeros(split, jnp.float32)
    total_im = jnp.zeros(split, jnp.float32)
    for block_id in range(BLOCKS):
        result = act_high(fields, ham_top[block_id, 0])
        result = act_mid(result, ham_mid[block_id])
        result = act_low(result, ham_low[block_id])
        result = act_high(result, ham_top[block_id, 1])
        flip = flip_masks[block_id]
        phase = phase_masks[block_id]
        signs = parity(devices, device_phase_masks[block_id])[:, :, None, None, None]
        signs = signs * parity(jnp.arange(TOP, dtype=jnp.int32), phase // (MID * LOW))[:, None, None]
        signs = signs * parity(jnp.arange(MID, dtype=jnp.int32), (phase // LOW) % MID)[:, None]
        signs = signs * parity(jnp.arange(LOW, dtype=jnp.int32), phase % LOW)
        index_a = jnp.bitwise_xor(jnp.arange(TOP, dtype=jnp.int32), flip // (MID * LOW))
        index_b = jnp.bitwise_xor(jnp.arange(MID, dtype=jnp.int32), (flip // LOW) % MID)
        index_c = jnp.bitwise_xor(jnp.arange(LOW, dtype=jnp.int32), flip % LOW)
        moved = []
        for piece in result:
            piece = piece.reshape(split) * signs
            piece = jnp.take(piece, index_a, axis=2)
            piece = jnp.take(piece, index_b, axis=3)
            piece = jnp.take(piece, index_c, axis=4)
            if flips_wide[block_id]:
                piece = jnp.roll(piece, N_WIDE // 2, axis=0)
            if flips_narrow[block_id]:
                piece = jnp.roll(piece, N_NARROW // 2, axis=1)
            moved.append(piece)
        total_re = total_re + moved[0]
        total_im = total_im + moved[1]
    cotangent = layout((total_re, total_im))
    return final_state, cotangent
```

```python
from functools import partial

import jax
import jax.numpy as jnp
from jax import lax
from jax.experimental import pallas as pl
from jax.experimental.pallas import tpu as pltpu
from jax.sharding import Mesh, PartitionSpec as P

TOP = 32
MID = 32
LOW = 64
ROUNDS = 3
BLOCKS = 3
XY = 16
HIGH = lax.Precision.HIGHEST
F32 = jnp.float32
BF16 = jnp.bfloat16


def split(value):
    high = value.astype(BF16)
    return high, (value - high.astype(F32)).astype(BF16)


def dot3(left, right):
    mul = partial(jnp.dot, preferred_element_type=F32)
    return mul(left[0], right[0]) + mul(left[1], right[0]) + mul(left[0], right[1])


def times_i(value):
    lane = lax.broadcasted_iota(jnp.int32, value.shape, 1)
    turned = pltpu.roll(value, LOW, 1)
    return jnp.where(lane < LOW, -turned, turned)


def iotas(shape):
    return lax.broadcasted_iota(jnp.int32, shape, 0), lax.broadcasted_iota(jnp.int32, shape, 1)


def sign_of(bits):
    for offset in (8, 4, 2, 1):
        bits = jnp.bitwise_xor(bits, jnp.right_shift(bits, offset))
    return (1 - 2 * jnp.bitwise_and(bits, 1)).astype(F32)


def hdot(left, right):
    return jnp.dot(left, right, precision=HIGH, preferred_element_type=F32)


def fold_left(order, flip, phase):
    row, col = iotas((order, order))
    return jnp.where(col == jnp.bitwise_xor(row, flip), sign_of(jnp.bitwise_and(col, phase)), 0.0)


def fold_right(order, flip, phase):
    row, col = iotas((order, order))
    return jnp.where(row == jnp.bitwise_xor(col, flip), sign_of(jnp.bitwise_and(row, phase)), 0.0)


def put(ref, index, value):
    high, low = split(value)
    ref[index, 0] = high
    ref[index, 1] = low


def prep_top(small_ref, where_ref, top_ref):
    zh = where_ref[1]
    total = hdot(hdot(small_ref[3], small_ref[2]), hdot(small_ref[1], small_ref[0]))
    row, col = iotas((TOP, 8 * XY))
    in_pick = jnp.where(row == 2 * (col // 8) + zh, 1.0, 0.0)
    wide = hdot(total[:, :TOP], in_pick)
    row, col = iotas((8 * XY, 8 * XY))
    same = jnp.where(row % 8 == col % 8, 1.0, 0.0)
    row, col = iotas((8 * XY, TOP))
    for index in range(2):
        pick = jnp.where(col == 2 * (row // 8) + (zh if index == 0 else 1 - zh), 1.0, 0.0)
        put(
            top_ref,
            index,
            jnp.concatenate([hdot(pick, wide[:TOP]) * same, hdot(pick, wide[TOP:]) * same], axis=1),
        )


def spread_high(matrix, scale):
    row, col = iotas((TOP, 8 * TOP))
    wide = hdot(matrix[:, :TOP], jnp.where(row == col // 8, 1.0, 0.0))
    row, col = iotas((8 * TOP, TOP))
    pick = jnp.where(col == row // 8, 1.0, 0.0)
    row, col = iotas((8 * TOP, 8 * TOP))
    same = jnp.where(row % 8 == col % 8, scale, 0.0)
    return jnp.concatenate([hdot(pick, wide[:TOP]) * same, hdot(pick, wide[TOP:]) * same], axis=1)


def spread_mid(matrix):
    row, col = iotas((MID, 4 * MID))
    wide = hdot(matrix[:, :MID], jnp.where(row == col % MID, 1.0, 0.0))
    row, col = iotas((4 * MID, MID))
    pick = jnp.where(col == row % MID, 1.0, 0.0)
    row, col = iotas((4 * MID, 4 * MID))
    same = jnp.where(row // MID == col // MID, 1.0, 0.0)
    return jnp.concatenate([hdot(pick, wide[:MID]) * same, hdot(pick, wide[MID:]) * same], axis=1)


def prep_blocks(small_ref, large_ref, masks_ref, where_ref, high_ref, mid_ref, low_ref):
    mid = hdot(hdot(small_ref[6], small_ref[5]), small_ref[4])
    low = hdot(hdot(large_ref[0], large_ref[1]), large_ref[2])
    put(mid_ref, BLOCKS, spread_mid(mid))
    put(low_ref, BLOCKS, jnp.concatenate([low, times_i(low)], axis=1))
    for block in range(BLOCKS):
        flip, phase = masks_ref[block], masks_ref[BLOCKS + block]
        source = where_ref[0] if block == 1 else jnp.bitwise_xor(where_ref[0], where_ref[2])
        scale = sign_of(jnp.bitwise_and(source, masks_ref[2 * BLOCKS + block]))
        fold = fold_left(2 * TOP, flip // (MID * LOW), phase // (MID * LOW))
        high = hdot(fold, hdot(small_ref[8 + 2 * block], small_ref[7 + 2 * block]))
        put(high_ref, block, spread_high(high, scale))
        fold = fold_left(2 * MID, flip // LOW % MID, phase // LOW % MID)
        put(mid_ref, block, spread_mid(hdot(fold, hdot(small_ref[13 + block], mid))))
        fold = fold_right(2 * LOW, flip % LOW, phase % LOW)
        full = hdot(hdot(low, large_ref[3 + block]), fold)
        put(low_ref, block, jnp.concatenate([full, times_i(full)], axis=1))


def top_kernel(field_ref, top_ref, own_ref, other_ref):
    for rest in range(2):
        for pair in range(2):
            parts = [
                field_ref[:, rest, 16 * pair + 8 * half : 16 * pair + 8 * half + 8, :].reshape(8 * XY, 2 * LOW)
                for half in range(2)
            ]
            right = jnp.concatenate(
                [jnp.concatenate(parts, axis=1), jnp.concatenate([times_i(part) for part in parts], axis=1)], axis=0
            )
            right = split(right)
            for index, out_ref in enumerate((own_ref, other_ref)):
                done = dot3((top_ref[index, 0], top_ref[index, 1]), right)
                for half in range(2):
                    out_ref[:, rest, 16 * pair + 8 * half : 16 * pair + 8 * half + 8, :] = done[
                        :, 2 * LOW * half : 2 * LOW * (half + 1)
                    ].reshape(XY, 8, 2 * LOW)


def add_kernel(own_ref, got_ref, out_ref):
    half = XY // 2
    total = own_ref[...] + got_ref[...]
    out_ref[:, 0] = total
    out_ref[:half, 1] = total[half:]
    out_ref[half:, 1] = total[:half]


def low_mid(load, mid, low, store):
    for group in range(4):
        done = dot3(split(load(group)), low)
        same, turned = done[:, : 2 * LOW], done[:, 2 * LOW :]
        right = jnp.concatenate(
            [
                jnp.concatenate([same[: 4 * MID], same[4 * MID :]], axis=1),
                jnp.concatenate([turned[: 4 * MID], turned[4 * MID :]], axis=1),
            ],
            axis=0,
        )
        done = dot3(mid, split(right))
        store(group, jnp.concatenate([done[:, : 2 * LOW], done[:, 2 * LOW :]], axis=0))


def pair_of(ref, index):
    return ref[index, 0], ref[index, 1]


def high_step(sources, matrices, out_ref):
    for pair in range(2):
        total = None
        for source_ref, matrix in zip(sources, matrices):
            parts = [
                source_ref[:, 16 * pair + 8 * half : 16 * pair + 8 * half + 8, :].reshape(8 * TOP, 2 * LOW)
                for half in range(2)
            ]
            right = jnp.concatenate(
                [jnp.concatenate(parts, axis=1), jnp.concatenate([times_i(part) for part in parts], axis=1)], axis=0
            )
            done = dot3(matrix, split(right))
            total = done if total is None else total + done
        for half in range(2):
            out_ref[:, 16 * pair + 8 * half : 16 * pair + 8 * half + 8, :] = total[
                :, 2 * LOW * half : 2 * LOW * (half + 1)
            ].reshape(TOP, 8, 2 * LOW)


def reader(field_ref, stream):
    return lambda group: field_ref[4 * group : 4 * group + 4, stream].reshape(8 * MID, 2 * LOW)


def writer(ref):
    def store(group, value):
        ref[8 * group : 8 * group + 8] = value.reshape(8, MID, 2 * LOW)

    return store


def send_kernel(field_ref, high_ref, mid_ref, low_ref, out_ref, first_ref, second_ref):
    low_mid(reader(field_ref, 0), pair_of(mid_ref, 1), pair_of(low_ref, 1), writer(first_ref))
    low_mid(reader(field_ref, 1), pair_of(mid_ref, 2), pair_of(low_ref, 2), writer(second_ref))
    high_step((first_ref, second_ref), (pair_of(high_ref, 1), pair_of(high_ref, 2)), out_ref)


def keep_kernel(field_ref, high_ref, mid_ref, low_ref, final_ref, out_ref, first_ref):
    low_mid(reader(field_ref, 1), pair_of(mid_ref, 0), pair_of(low_ref, 0), writer(first_ref))
    high_step((first_ref,), (pair_of(high_ref, 0),), out_ref)
    low_mid(reader(field_ref, 0), pair_of(mid_ref, 3), pair_of(low_ref, 3), writer(final_ref))


def real_form(matrix):
    real, imag = matrix[:, 0], matrix[:, 1]
    return jnp.concatenate(
        [jnp.concatenate([real, -imag], axis=2), jnp.concatenate([imag, real], axis=2)], axis=1
    )


def flat_form(matrix):
    real, imag = jnp.swapaxes(matrix[:, 0], 1, 2), jnp.swapaxes(matrix[:, 1], 1, 2)
    return jnp.concatenate(
        [jnp.concatenate([real, imag], axis=2), jnp.concatenate([-imag, real], axis=2)], axis=1
    )


def vm():
    return pl.BlockSpec(memory_space=pltpu.VMEM)


def sm():
    return pl.BlockSpec(memory_space=pltpu.SMEM)


def call(body, ins, outs, scratch=(), smem=(), name=None):
    return pl.pallas_call(
        body,
        in_specs=[sm() if i in smem else vm() for i in range(ins)],
        out_specs=[vm() for _ in outs],
        out_shape=[jax.ShapeDtypeStruct(s, t) for s, t in outs],
        scratch_shapes=[pltpu.VMEM(s, t) for s, t in scratch],
        compiler_params=pltpu.CompilerParams(vmem_limit_bytes=48 * 2**20),
        name=name,
    )


def shards(
    amplitudes,
    top_gates,
    mid_gates,
    low_gates,
    ham_top,
    ham_mid,
    ham_low,
    flip_masks,
    phase_masks,
    device_phase_masks,
):
    width = 2 * LOW
    inside = lax.all_to_all(
        amplitudes.reshape(XY, 2 * MID, width), ("x", "y"), split_axis=0, concat_axis=0, tiled=True
    ).reshape(XY, 2, MID, width)
    small = real_form(
        jnp.concatenate([top_gates, mid_gates, ham_top.reshape(2 * BLOCKS, 2, TOP, TOP), ham_mid], axis=0)
    )
    large = flat_form(jnp.concatenate([low_gates, ham_low], axis=0))
    zh = lax.axis_index("zh")
    n = lax.axis_index("narrow")
    device_id = ((lax.axis_index("x") * 4 + lax.axis_index("y")) * 2 + zh) * 8 + n
    where = jnp.stack([device_id, zh, jnp.int32(16 * 8)]).astype(jnp.int32)
    masks = jnp.concatenate([flip_masks, phase_masks, device_phase_masks])
    (top,) = call(prep_top, 2, [((2, 2, 128, 256), BF16)], smem=(1,), name="prep_top")(small, where)
    high, mid, low = call(
        prep_blocks,
        4,
        [((3, 2, 256, 512), BF16), ((4, 2, 128, 256), BF16), ((4, 2, 128, 256), BF16)],
        smem=(2, 3),
        name="prep_blocks",
    )(small, large, masks, where)
    piece = ((XY, 2, MID, width), F32)
    own, other = call(top_kernel, 2, [piece, piece], name="top")(inside, top)
    got = lax.ppermute(other, "zh", [(0, 1), (1, 0)])
    (both,) = call(add_kernel, 2, [((XY, 2, 2, MID, width), F32)], name="add")(own, got)
    field = lax.all_to_all(
        both.reshape(XY, 4 * MID, width), ("x", "y"), split_axis=0, concat_axis=0, tiled=True
    ).reshape(XY, 2, 2, MID, width)
    whole = ((TOP, MID, width), F32)
    (sent,) = call(send_kernel, 4, [whole], [whole, whole], name="send")(field, high, mid, low)
    arrived = lax.ppermute(sent, "narrow", [(i, i ^ 4) for i in range(8)])
    final, kept = call(keep_kernel, 4, [whole, whole], [whole], name="keep")(field, high, mid, low)
    cotangent = kept + arrived
    return final.reshape(TOP * MID, width), cotangent.reshape(TOP * MID, width)


def solution(mesh):
    fine = Mesh(mesh.devices.reshape(4, 4, 2, 8), ("x", "y", "zh", "narrow"))
    rows = P(("x", "y", "zh", "narrow"), None)
    return jax.shard_map(
        shards,
        mesh=fine,
        in_specs=(rows, P(), P(), P(), P(), P(), P(), P(), P(), P()),
        out_specs=(rows, rows),
        check_vma=False,
    )
```

```python
import jax
import jax.numpy as jnp
from jax import lax
from jax.experimental import pallas as pl
from jax.experimental.pallas import tpu as pltpu
from jax.sharding import Mesh, PartitionSpec as P


TOP = 32
MID = 32
LOW = 64
BLOCKS = 3
XY = 16
EARLY = 8
HIGH = lax.Precision.HIGHEST
F32 = jnp.float32
BF16 = jnp.bfloat16


def split(value):
    high = value.astype(BF16)
    return high, (value - high.astype(F32)).astype(BF16)


def dot3(left, right):
    high, low = left
    upper, lower = right
    return jnp.dot(
        jnp.concatenate([high, low, high], axis=1),
        jnp.concatenate([upper, upper, lower], axis=0),
        preferred_element_type=F32,
    )


def times_i(value):
    lane = lax.broadcasted_iota(jnp.int32, value.shape, 1)
    turned = pltpu.roll(value, LOW, 1)
    return jnp.where(lane < LOW, -turned, turned)


def iotas(shape):
    return lax.broadcasted_iota(jnp.int32, shape, 0), lax.broadcasted_iota(jnp.int32, shape, 1)


def sign_of(bits):
    for offset in (8, 4, 2, 1):
        bits = jnp.bitwise_xor(bits, jnp.right_shift(bits, offset))
    return (1 - 2 * jnp.bitwise_and(bits, 1)).astype(F32)


def hdot(left, right):
    return jnp.dot(left, right, precision=HIGH, preferred_element_type=F32)


def fold_left(order, flip, phase):
    row, col = iotas((order, order))
    return jnp.where(col == jnp.bitwise_xor(row, flip), sign_of(jnp.bitwise_and(col, phase)), 0.0)


def fold_right(order, flip, phase):
    row, col = iotas((order, order))
    return jnp.where(row == jnp.bitwise_xor(col, flip), sign_of(jnp.bitwise_and(row, phase)), 0.0)


def put(ref, index, value):
    high, low = split(value)
    ref[index, 0] = high
    ref[index, 1] = low


def prep_top(small_ref, where_ref, top_ref):
    zh = where_ref[1]
    total = hdot(hdot(small_ref[3], small_ref[2]), hdot(small_ref[1], small_ref[0]))
    row, col = iotas((TOP, 8 * XY))
    in_pick = jnp.where(row == 2 * (col // 8) + zh, 1.0, 0.0)
    wide = hdot(total[:, :TOP], in_pick)
    row, col = iotas((8 * XY, 8 * XY))
    same = jnp.where(row % 8 == col % 8, 1.0, 0.0)
    row, col = iotas((8 * XY, TOP))
    for index in range(2):
        pick = jnp.where(col == 2 * (row // 8) + (zh if index == 0 else 1 - zh), 1.0, 0.0)
        put(
            top_ref,
            index,
            jnp.concatenate([hdot(pick, wide[:TOP]) * same, hdot(pick, wide[TOP:]) * same], axis=1),
        )


def spread_high(matrix, scale):
    row, col = iotas((TOP, 8 * TOP))
    wide = hdot(matrix[:, :TOP], jnp.where(row == col // 8, 1.0, 0.0))
    row, col = iotas((8 * TOP, TOP))
    pick = jnp.where(col == row // 8, 1.0, 0.0)
    row, col = iotas((8 * TOP, 8 * TOP))
    same = jnp.where(row % 8 == col % 8, scale, 0.0)
    return jnp.concatenate([hdot(pick, wide[:TOP]) * same, hdot(pick, wide[TOP:]) * same], axis=0)


def spread_mid(matrix):
    row, col = iotas((MID, 4 * MID))
    wide = hdot(matrix[:, :MID], jnp.where(row == col % MID, 1.0, 0.0))
    row, col = iotas((4 * MID, MID))
    pick = jnp.where(col == row % MID, 1.0, 0.0)
    row, col = iotas((4 * MID, 4 * MID))
    same = jnp.where(row // MID == col // MID, 1.0, 0.0)
    return jnp.concatenate([hdot(pick, wide[:MID]) * same, hdot(pick, wide[MID:]) * same], axis=1)


def prep_block(refs, block, slot, mid, low):
    small_ref, large_ref, masks_ref, where_ref, high_ref, mid_ref, low_ref = refs
    flip, phase = masks_ref[block], masks_ref[BLOCKS + block]
    source = where_ref[0] if block == 1 else jnp.bitwise_xor(where_ref[0], where_ref[2])
    scale = sign_of(jnp.bitwise_and(source, masks_ref[2 * BLOCKS + block]))
    fold = fold_left(2 * TOP, flip // (MID * LOW), phase // (MID * LOW))
    high = hdot(fold, hdot(small_ref[8 + 2 * block], small_ref[7 + 2 * block]))
    put(high_ref, slot, spread_high(high, scale))
    fold = fold_left(2 * MID, flip // LOW % MID, phase // LOW % MID)
    put(mid_ref, slot, spread_mid(hdot(fold, hdot(small_ref[13 + block], mid))))
    fold = fold_right(2 * LOW, flip % LOW, phase % LOW)
    full = hdot(hdot(low, large_ref[3 + block]), fold)
    put(low_ref, slot, jnp.concatenate([full, times_i(full)], axis=1))


def merged(small_ref, large_ref):
    mid = hdot(hdot(small_ref[6], small_ref[5]), small_ref[4])
    return mid, hdot(hdot(large_ref[0], large_ref[1]), large_ref[2])


def prep_send(small_ref, large_ref, masks_ref, where_ref, high_ref, mid_ref, low_ref, built_ref, sems):
    mid, low = merged(small_ref, large_ref)
    refs = (small_ref, large_ref, masks_ref, where_ref, built_ref, mid_ref, low_ref)
    copies = [pltpu.make_async_copy(built_ref.at[slot], high_ref.at[slot], sems.at[slot]) for slot in range(2)]
    for slot in range(2):
        prep_block(refs, slot + 1, slot, mid, low)
        copies[slot].start()
    for copy in copies:
        copy.wait()


def prep_keep(*refs):
    mid, low = merged(*refs[:2])
    prep_block(refs, 0, 0, mid, low)
    put(refs[5], 1, spread_mid(mid))
    put(refs[6], 1, jnp.concatenate([low, times_i(low)], axis=1))


def two_streams(out_ref, first, value):
    half = XY // 2
    out_ref[:, first] = value
    out_ref[:half, first + 1] = value[half:]
    out_ref[half:, first + 1] = value[:half]


def top_kernel(field_ref, top_ref, own_ref, other_ref, early_ref):
    for rest in range(2):
        for pair in range(2):
            parts = [
                field_ref[:, rest, 16 * pair + 8 * half : 16 * pair + 8 * half + 8, :].reshape(8 * XY, 2 * LOW)
                for half in range(2)
            ]
            right = jnp.concatenate(
                [jnp.concatenate(parts, axis=1), jnp.concatenate([times_i(part) for part in parts], axis=1)], axis=0
            )
            right = split(right)
            for index, out_ref in enumerate((own_ref, other_ref)):
                done = dot3((top_ref[index, 0], top_ref[index, 1]), right)
                for half in range(2):
                    group = 2 * pair + half
                    value = done[:, 2 * LOW * half : 2 * LOW * (half + 1)].reshape(XY, 8, 2 * LOW)
                    if group == 0:
                        two_streams(early_ref.at[:, :, rest], 2 * index, value)
                    else:
                        out_ref[:, rest, 8 * group - EARLY : 8 * group - EARLY + 8, :] = value


def add_kernel(own_ref, got_ref, out_ref):
    two_streams(out_ref, 0, own_ref[...] + got_ref[...])


def low_mid(load, mid, low, store):
    for group in range(4):
        done = dot3(split(load(group)), low)
        same, turned = done[:, : 2 * LOW], done[:, 2 * LOW :]
        right = jnp.concatenate(
            [
                jnp.concatenate([same[: 4 * MID], same[4 * MID :]], axis=1),
                jnp.concatenate([turned[: 4 * MID], turned[4 * MID :]], axis=1),
            ],
            axis=0,
        )
        done = dot3(mid, split(right))
        store(group, jnp.concatenate([done[:, : 2 * LOW], done[:, 2 * LOW :]], axis=0))


def pair_of(ref, index):
    return ref[index, 0], ref[index, 1]


def high_step(sources, matrices, out_ref):
    rows = 8 * TOP
    for pair in range(2):
        total = None
        for source_ref, matrix in zip(sources, matrices):
            parts = [
                source_ref[:, 16 * pair + 8 * half : 16 * pair + 8 * half + 8, :].reshape(rows, 2 * LOW)
                for half in range(2)
            ]
            done = dot3(matrix, split(jnp.concatenate(parts, axis=1)))
            total = done if total is None else total + done
        for half in range(2):
            part = total[:, 2 * LOW * half : 2 * LOW * (half + 1)]
            value = part[:rows] + times_i(part[rows:])
            out_ref[:, 16 * pair + 8 * half : 16 * pair + 8 * half + 8, :] = value.reshape(TOP, 8, 2 * LOW)


def reader(fields, stream):
    early_ref, got_ref, late_ref = fields

    def load(group):
        part = slice(4 * group, 4 * group + 4)
        early = early_ref[part, stream] + got_ref[part, stream]
        return jnp.concatenate(
            [early.reshape(8, EARLY, 2 * LOW), late_ref[part, stream].reshape(8, MID - EARLY, 2 * LOW)], axis=1
        ).reshape(8 * MID, 2 * LOW)

    return load


def writer(ref):
    def store(group, value):
        ref[8 * group : 8 * group + 8] = value.reshape(8, MID, 2 * LOW)

    return store


def send_kernel(early_ref, got_ref, late_ref, high_ref, mid_ref, low_ref, out_ref, first_ref, second_ref, held_ref, sems):
    fields = (early_ref, got_ref, late_ref)
    copies = [pltpu.make_async_copy(high_ref.at[slot], held_ref.at[slot], sems.at[slot]) for slot in range(2)]
    for copy in copies:
        copy.start()
    low_mid(reader(fields, 0), pair_of(mid_ref, 0), pair_of(low_ref, 0), writer(first_ref))
    low_mid(reader(fields, 1), pair_of(mid_ref, 1), pair_of(low_ref, 1), writer(second_ref))
    for copy in copies:
        copy.wait()
    high_step((first_ref, second_ref), (pair_of(held_ref, 0), pair_of(held_ref, 1)), out_ref)


def keep_kernel(early_ref, got_ref, late_ref, high_ref, mid_ref, low_ref, final_ref, out_ref, first_ref):
    fields = (early_ref, got_ref, late_ref)
    low_mid(reader(fields, 1), pair_of(mid_ref, 0), pair_of(low_ref, 0), writer(first_ref))
    high_step((first_ref,), (pair_of(high_ref, 0),), out_ref)
    low_mid(reader(fields, 0), pair_of(mid_ref, 1), pair_of(low_ref, 1), writer(final_ref))


def real_form(matrix):
    real, imag = matrix[:, 0], matrix[:, 1]
    return jnp.concatenate(
        [jnp.concatenate([real, -imag], axis=2), jnp.concatenate([imag, real], axis=2)], axis=1
    )


def flat_form(matrix):
    real, imag = jnp.swapaxes(matrix[:, 0], 1, 2), jnp.swapaxes(matrix[:, 1], 1, 2)
    return jnp.concatenate(
        [jnp.concatenate([real, imag], axis=2), jnp.concatenate([-imag, real], axis=2)], axis=1
    )


def vm():
    return pl.BlockSpec(memory_space=pltpu.VMEM)


def sm():
    return pl.BlockSpec(memory_space=pltpu.SMEM)


def call(body, ins, outs, scratch=(), smem=(), far_in=(), far_out=(), copies=0):
    far = pl.BlockSpec(memory_space=pltpu.HBM)
    held = [pltpu.VMEM(s, t) for s, t in scratch]
    if copies:
        held.append(pltpu.SemaphoreType.DMA((copies,)))
    return pl.pallas_call(
        body,
        in_specs=[sm() if i in smem else far if i in far_in else vm() for i in range(ins)],
        out_specs=[far if i in far_out else vm() for i in range(len(outs))],
        out_shape=[jax.ShapeDtypeStruct(s, t) for s, t in outs],
        scratch_shapes=held,
        compiler_params=pltpu.CompilerParams(vmem_limit_bytes=16 * 2**20),
    )


def evolve(
    amplitudes,
    top_gates,
    mid_gates,
    low_gates,
    ham_top,
    ham_mid,
    ham_low,
    flip_masks,
    phase_masks,
    device_phase_masks,
):
    width = 2 * LOW
    inside = lax.all_to_all(
        amplitudes.reshape(XY, 2 * MID, width), ("x", "y"), split_axis=0, concat_axis=0, tiled=True
    ).reshape(XY, 2, MID, width)
    small = real_form(
        jnp.concatenate([top_gates, mid_gates, ham_top.reshape(2 * BLOCKS, 2, TOP, TOP), ham_mid], axis=0)
    )
    large = flat_form(jnp.concatenate([low_gates, ham_low], axis=0))
    zh = lax.axis_index("zh")
    n = lax.axis_index("narrow")
    device_id = ((lax.axis_index("x") * 4 + lax.axis_index("y")) * 2 + zh) * 8 + n
    where = jnp.stack([device_id, zh, jnp.int32(16 * 8)]).astype(jnp.int32)
    masks = jnp.concatenate([flip_masks, phase_masks, device_phase_masks])
    (top,) = call(prep_top, 2, [((2, 2, 128, 256), BF16)], smem=(1,))(small, where)
    late = MID - EARLY
    piece = ((XY, 2, late, width), F32)
    own, other, early = call(top_kernel, 2, [piece, piece, ((XY, 4, 2, EARLY, width), F32)])(inside, top)
    swap = [(0, 1), (1, 0)]
    got = lax.ppermute(other, "zh", swap)
    early = lax.all_to_all(
        early.reshape(XY, 8 * EARLY, width), ("x", "y"), split_axis=0, concat_axis=0, tiled=True
    ).reshape(XY, 4, 2, EARLY, width)
    prepared = [((2, 2, 512, 256), BF16), ((2, 2, 128, 256), BF16), ((2, 2, 128, 256), BF16)]
    high, mid, low = call(
        prep_send, 4, prepared, prepared[:1], smem=(2, 3), far_out=(0,), copies=2
    )(small, large, masks, where)
    early_got = lax.ppermute(early[:, 2:], "zh", swap)
    (both,) = call(add_kernel, 2, [((XY, 2, 2, late, width), F32)])(own, got)
    field = lax.all_to_all(
        both.reshape(XY, 4 * late, width), ("x", "y"), split_axis=0, concat_axis=0, tiled=True
    ).reshape(XY, 2, 2, late, width)
    whole = ((TOP, MID, width), F32)
    fields = (early, early_got, field)
    (sent,) = call(
        send_kernel, 6, [whole], [whole, whole] + prepared[:1], far_in=(3,), copies=2
    )(*fields, high, mid, low)
    arrived = lax.ppermute(sent, "narrow", [(i, i ^ 4) for i in range(8)])
    prepared = [((1, 2, 512, 256), BF16)] + prepared[1:]
    high, mid, low = call(prep_keep, 4, prepared, smem=(2, 3))(small, large, masks, where)
    final, kept = call(keep_kernel, 6, [whole, whole], [whole])(*fields, high, mid, low)
    cotangent = kept + arrived
    return final.reshape(TOP * MID, width), cotangent.reshape(TOP * MID, width)


def solution(mesh):
    fine = Mesh(mesh.devices.reshape(4, 4, 2, 8), ("x", "y", "zh", "narrow"))
    rows = P(("x", "y", "zh", "narrow"), None)
    return jax.shard_map(
        evolve,
        mesh=fine,
        in_specs=(rows, P(), P(), P(), P(), P(), P(), P(), P(), P()),
        out_specs=(rows, rows),
        check_vma=False,
    )
```

```python
import jax
import jax.numpy as jnp
from jax import lax
from jax.experimental import pallas as pl
from jax.experimental.pallas import tpu as pltpu
from jax.sharding import Mesh, PartitionSpec as P


TOP = 32
MID = 32
LOW = 64
BLOCKS = 3
XY = 16
EARLY = 8
HIGH = lax.Precision.HIGHEST
F32 = jnp.float32
BF16 = jnp.bfloat16


def split(value):
    high = value.astype(BF16)
    return high, (value - high.astype(F32)).astype(BF16)


def dot3(left, right):
    high, low = left
    upper, lower = right
    return jnp.dot(
        jnp.concatenate([high, low, high], axis=1),
        jnp.concatenate([upper, upper, lower], axis=0),
        preferred_element_type=F32,
    )


def times_i(value):
    lane = lax.broadcasted_iota(jnp.int32, value.shape, 1)
    turned = pltpu.roll(value, LOW, 1)
    return jnp.where(lane < LOW, -turned, turned)


def iotas(shape):
    return lax.broadcasted_iota(jnp.int32, shape, 0), lax.broadcasted_iota(jnp.int32, shape, 1)


def sign_of(bits):
    for offset in (8, 4, 2, 1):
        bits = jnp.bitwise_xor(bits, jnp.right_shift(bits, offset))
    return (1 - 2 * jnp.bitwise_and(bits, 1)).astype(F32)


def hdot(left, right):
    return jnp.dot(left, right, precision=HIGH, preferred_element_type=F32)


def fold_left(order, flip, phase):
    row, col = iotas((order, order))
    return jnp.where(col == jnp.bitwise_xor(row, flip), sign_of(jnp.bitwise_and(col, phase)), 0.0)


def fold_right(order, flip, phase):
    row, col = iotas((order, order))
    return jnp.where(row == jnp.bitwise_xor(col, flip), sign_of(jnp.bitwise_and(row, phase)), 0.0)


def put(ref, index, value):
    high, low = split(value)
    ref[index, 0] = high
    ref[index, 1] = low


def prep_top(small_ref, where_ref, top_ref):
    zh = where_ref[1]
    total = hdot(hdot(small_ref[3], small_ref[2]), hdot(small_ref[1], small_ref[0]))
    row, col = iotas((TOP, 8 * XY))
    in_pick = jnp.where(row == 2 * (col // 8) + zh, 1.0, 0.0)
    wide = hdot(total[:, :TOP], in_pick)
    row, col = iotas((8 * XY, 8 * XY))
    same = jnp.where(row % 8 == col % 8, 1.0, 0.0)
    row, col = iotas((8 * XY, TOP))
    for index in range(2):
        pick = jnp.where(col == 2 * (row // 8) + (zh if index == 0 else 1 - zh), 1.0, 0.0)
        put(
            top_ref,
            index,
            jnp.concatenate([hdot(pick, wide[:TOP]) * same, hdot(pick, wide[TOP:]) * same], axis=1),
        )


def spread_high(matrix, scale):
    row, col = iotas((TOP, 8 * TOP))
    wide = hdot(matrix[:, :TOP], jnp.where(row == col // 8, 1.0, 0.0))
    row, col = iotas((8 * TOP, TOP))
    pick = jnp.where(col == row // 8, 1.0, 0.0)
    row, col = iotas((8 * TOP, 8 * TOP))
    same = jnp.where(row % 8 == col % 8, scale, 0.0)
    return jnp.concatenate([hdot(pick, wide[:TOP]) * same, hdot(pick, wide[TOP:]) * same], axis=0)


def spread_mid(matrix):
    row, col = iotas((MID, 4 * MID))
    wide = hdot(matrix[:, :MID], jnp.where(row == col % MID, 1.0, 0.0))
    row, col = iotas((4 * MID, MID))
    pick = jnp.where(col == row % MID, 1.0, 0.0)
    row, col = iotas((4 * MID, 4 * MID))
    same = jnp.where(row // MID == col // MID, 1.0, 0.0)
    return jnp.concatenate([hdot(pick, wide[:MID]) * same, hdot(pick, wide[MID:]) * same], axis=1)


def prep_block(refs, block, slot, mid, low):
    small_ref, large_ref, masks_ref, where_ref, high_ref, mid_ref, low_ref = refs
    flip, phase = masks_ref[block], masks_ref[BLOCKS + block]
    source = where_ref[0] if block == 1 else jnp.bitwise_xor(where_ref[0], where_ref[2])
    scale = sign_of(jnp.bitwise_and(source, masks_ref[2 * BLOCKS + block]))
    fold = fold_left(2 * TOP, flip // (MID * LOW), phase // (MID * LOW))
    high = hdot(fold, hdot(small_ref[8 + 2 * block], small_ref[7 + 2 * block]))
    put(high_ref, slot, spread_high(high, scale))
    fold = fold_left(2 * MID, flip // LOW % MID, phase // LOW % MID)
    put(mid_ref, slot, spread_mid(hdot(fold, hdot(small_ref[13 + block], mid))))
    fold = fold_right(2 * LOW, flip % LOW, phase % LOW)
    full = hdot(hdot(low, large_ref[3 + block]), fold)
    put(low_ref, slot, jnp.concatenate([full, times_i(full)], axis=1))


def merged(small_ref, large_ref):
    mid = hdot(hdot(small_ref[6], small_ref[5]), small_ref[4])
    return mid, hdot(hdot(large_ref[0], large_ref[1]), large_ref[2])


def parts_of(ref):
    return ref.at[:, :, :512], ref.at[:, :, 512:640], ref.at[:, :, 640:]


def prep_send(small_ref, large_ref, masks_ref, where_ref, out_ref):
    mid, low = merged(small_ref, large_ref)
    for slot in range(2):
        prep_block((small_ref, large_ref, masks_ref, where_ref) + parts_of(out_ref), slot + 1, slot, mid, low)


def prep_keep(*refs):
    mid, low = merged(*refs[:2])
    prep_block(refs, 0, 0, mid, low)
    put(refs[5], 1, spread_mid(mid))
    put(refs[6], 1, jnp.concatenate([low, times_i(low)], axis=1))


def two_streams(out_ref, first, value):
    half = XY // 2
    out_ref[:, first] = value
    out_ref[:half, first + 1] = value[half:]
    out_ref[half:, first + 1] = value[:half]


def top_kernel(field_ref, top_ref, own_ref, other_ref, early_ref):
    for rest in range(2):
        for pair in range(2):
            parts = [
                field_ref[:, rest, 16 * pair + 8 * half : 16 * pair + 8 * half + 8, :].reshape(8 * XY, 2 * LOW)
                for half in range(2)
            ]
            right = jnp.concatenate(
                [jnp.concatenate(parts, axis=1), jnp.concatenate([times_i(part) for part in parts], axis=1)], axis=0
            )
            right = split(right)
            for index, out_ref in enumerate((own_ref, other_ref)):
                done = dot3((top_ref[index, 0], top_ref[index, 1]), right)
                for half in range(2):
                    group = 2 * pair + half
                    value = done[:, 2 * LOW * half : 2 * LOW * (half + 1)].reshape(XY, 8, 2 * LOW)
                    if group == 0:
                        two_streams(early_ref.at[:, :, rest], 2 * index, value)
                    else:
                        out_ref[:, rest, 8 * group - EARLY : 8 * group - EARLY + 8, :] = value


def add_kernel(own_ref, got_ref, out_ref):
    two_streams(out_ref, 0, own_ref[...] + got_ref[...])


def low_mid(load, mid, low, store):
    for group in range(4):
        done = dot3(split(load(group)), low)
        same, turned = done[:, : 2 * LOW], done[:, 2 * LOW :]
        right = jnp.concatenate(
            [
                jnp.concatenate([same[: 4 * MID], same[4 * MID :]], axis=1),
                jnp.concatenate([turned[: 4 * MID], turned[4 * MID :]], axis=1),
            ],
            axis=0,
        )
        done = dot3(mid, split(right))
        store(group, jnp.concatenate([done[:, : 2 * LOW], done[:, 2 * LOW :]], axis=0))


def pair_of(ref, index):
    return ref[index, 0], ref[index, 1]


def high_step(sources, matrices, out_ref):
    rows = 8 * TOP
    for pair in range(2):
        total = None
        for source_ref, matrix in zip(sources, matrices):
            parts = [
                source_ref[:, 16 * pair + 8 * half : 16 * pair + 8 * half + 8, :].reshape(rows, 2 * LOW)
                for half in range(2)
            ]
            done = dot3(matrix, split(jnp.concatenate(parts, axis=1)))
            total = done if total is None else total + done
        for half in range(2):
            part = total[:, 2 * LOW * half : 2 * LOW * (half + 1)]
            value = part[:rows] + times_i(part[rows:])
            out_ref[:, 16 * pair + 8 * half : 16 * pair + 8 * half + 8, :] = value.reshape(TOP, 8, 2 * LOW)


def reader(fields, stream):
    early_ref, got_ref, late_ref = fields

    def load(group):
        part = slice(4 * group, 4 * group + 4)
        early = early_ref[part, stream] + got_ref[part, stream]
        return jnp.concatenate(
            [early.reshape(8, EARLY, 2 * LOW), late_ref[part, stream].reshape(8, MID - EARLY, 2 * LOW)], axis=1
        ).reshape(8 * MID, 2 * LOW)

    return load


def writer(ref):
    def store(group, value):
        ref[8 * group : 8 * group + 8] = value.reshape(8, MID, 2 * LOW)

    return store


def send_kernel(early_ref, got_ref, late_ref, built_ref, out_ref, first_ref, second_ref):
    fields = (early_ref, got_ref, late_ref)
    high_ref, mid_ref, low_ref = parts_of(built_ref)
    for slot, half_ref in enumerate((first_ref, second_ref)):
        low_mid(reader(fields, slot), pair_of(mid_ref, slot), pair_of(low_ref, slot), writer(half_ref))
    high_step((first_ref, second_ref), (pair_of(high_ref, 0), pair_of(high_ref, 1)), out_ref)


def keep_kernel(early_ref, got_ref, late_ref, high_ref, mid_ref, low_ref, final_ref, out_ref, first_ref):
    fields = (early_ref, got_ref, late_ref)
    low_mid(reader(fields, 1), pair_of(mid_ref, 0), pair_of(low_ref, 0), writer(first_ref))
    high_step((first_ref,), (pair_of(high_ref, 0),), out_ref)
    low_mid(reader(fields, 0), pair_of(mid_ref, 1), pair_of(low_ref, 1), writer(final_ref))


def real_form(matrix):
    real, imag = matrix[:, 0], matrix[:, 1]
    return jnp.concatenate(
        [jnp.concatenate([real, -imag], axis=2), jnp.concatenate([imag, real], axis=2)], axis=1
    )


def flat_form(matrix):
    real, imag = jnp.swapaxes(matrix[:, 0], 1, 2), jnp.swapaxes(matrix[:, 1], 1, 2)
    return jnp.concatenate(
        [jnp.concatenate([real, imag], axis=2), jnp.concatenate([-imag, real], axis=2)], axis=1
    )


def vm():
    return pl.BlockSpec(memory_space=pltpu.VMEM)


def sm():
    return pl.BlockSpec(memory_space=pltpu.SMEM)


def call(body, ins, outs, scratch=(), smem=()):
    return pl.pallas_call(
        body,
        in_specs=[sm() if i in smem else vm() for i in range(ins)],
        out_specs=[vm() for _ in outs],
        out_shape=[jax.ShapeDtypeStruct(s, t) for s, t in outs],
        scratch_shapes=[pltpu.VMEM(s, t) for s, t in scratch],
        compiler_params=pltpu.CompilerParams(vmem_limit_bytes=16 * 2**20),
    )


def evolve(
    amplitudes,
    top_gates,
    mid_gates,
    low_gates,
    ham_top,
    ham_mid,
    ham_low,
    flip_masks,
    phase_masks,
    device_phase_masks,
):
    width = 2 * LOW
    inside = lax.all_to_all(
        amplitudes.reshape(XY, 2 * MID, width), ("x", "y"), split_axis=0, concat_axis=0, tiled=True
    ).reshape(XY, 2, MID, width)
    small = real_form(
        jnp.concatenate([top_gates, mid_gates, ham_top.reshape(2 * BLOCKS, 2, TOP, TOP), ham_mid], axis=0)
    )
    large = flat_form(jnp.concatenate([low_gates, ham_low], axis=0))
    zh = lax.axis_index("zh")
    n = lax.axis_index("narrow")
    device_id = ((lax.axis_index("x") * 4 + lax.axis_index("y")) * 2 + zh) * 8 + n
    where = jnp.stack([device_id, zh, jnp.int32(16 * 8)]).astype(jnp.int32)
    masks = jnp.concatenate([flip_masks, phase_masks, device_phase_masks])
    (top,) = call(prep_top, 2, [((2, 2, 128, 256), BF16)], smem=(1,))(small, where)
    late = MID - EARLY
    piece = ((XY, 2, late, width), F32)
    own, other, early = call(top_kernel, 2, [piece, piece, ((XY, 4, 2, EARLY, width), F32)])(inside, top)
    swap = [(0, 1), (1, 0)]
    got = lax.ppermute(other, "zh", swap)
    early = lax.all_to_all(
        early.reshape(XY, 8 * EARLY, width), ("x", "y"), split_axis=0, concat_axis=0, tiled=True
    ).reshape(XY, 4, 2, EARLY, width)
    early_got = lax.ppermute(early[:, 2:], "zh", swap)
    (both,) = call(add_kernel, 2, [((XY, 2, 2, late, width), F32)])(own, got)
    field = lax.all_to_all(
        both.reshape(XY, 4 * late, width), ("x", "y"), split_axis=0, concat_axis=0, tiled=True
    ).reshape(XY, 2, 2, late, width)
    operators = ((2, 2, 768, 256), BF16)
    (built,) = call(prep_send, 4, [operators], smem=(2, 3))(small, large, masks, where)
    whole = ((TOP, MID, width), F32)
    fields = (early, early_got, field)
    (sent,) = call(send_kernel, 4, [whole], [whole, whole])(*fields, built)
    arrived = lax.ppermute(sent, "narrow", [(i, i ^ 4) for i in range(8)])
    prepared = [((1, 2, 512, 256), BF16), ((2, 2, 128, 256), BF16), ((2, 2, 128, 256), BF16)]
    high, mid, low = call(prep_keep, 4, prepared, smem=(2, 3))(small, large, masks, where)
    final, kept = call(keep_kernel, 6, [whole, whole], [whole])(*fields, high, mid, low)
    cotangent = kept + arrived
    return final.reshape(TOP * MID, width), cotangent.reshape(TOP * MID, width)


def solution(mesh):
    fine = Mesh(mesh.devices.reshape(4, 4, 2, 8), ("x", "y", "zh", "narrow"))
    rows = P(("x", "y", "zh", "narrow"), None)
    return jax.shard_map(
        evolve,
        mesh=fine,
        in_specs=(rows, P(), P(), P(), P(), P(), P(), P(), P(), P()),
        out_specs=(rows, rows),
        check_vma=False,
    )
```

```python
import jax
import jax.numpy as jnp
from jax import lax
from jax.experimental import pallas as pl
from jax.experimental.pallas import tpu as pltpu
from jax.sharding import Mesh, PartitionSpec as P


TOP = 32
MID = 32
LOW = 64
BLOCKS = 3
XY = 16
EARLY = 8
HIGH = lax.Precision.HIGHEST
F32 = jnp.float32
BF16 = jnp.bfloat16


def split(value):
    high = value.astype(BF16)
    return high, (value - high.astype(F32)).astype(BF16)


def dot3(left, right):
    high, low = left
    upper, lower = right
    return jnp.dot(
        jnp.concatenate([high, low, high], axis=1),
        jnp.concatenate([upper, upper, lower], axis=0),
        preferred_element_type=F32,
    )


def times_i(value):
    lane = lax.broadcasted_iota(jnp.int32, value.shape, 1)
    turned = pltpu.roll(value, LOW, 1)
    return jnp.where(lane < LOW, -turned, turned)


def iotas(shape):
    return lax.broadcasted_iota(jnp.int32, shape, 0), lax.broadcasted_iota(jnp.int32, shape, 1)


def sign_of(bits):
    for offset in (8, 4, 2, 1):
        bits = jnp.bitwise_xor(bits, jnp.right_shift(bits, offset))
    return (1 - 2 * jnp.bitwise_and(bits, 1)).astype(F32)


def hdot(left, right):
    return jnp.dot(left, right, precision=HIGH, preferred_element_type=F32)


def fold_left(order, flip, phase):
    row, col = iotas((order, order))
    return jnp.where(col == jnp.bitwise_xor(row, flip), sign_of(jnp.bitwise_and(col, phase)), 0.0)


def fold_right(order, flip, phase):
    row, col = iotas((order, order))
    return jnp.where(row == jnp.bitwise_xor(col, flip), sign_of(jnp.bitwise_and(row, phase)), 0.0)


def put(ref, index, value):
    high, low = split(value)
    ref[index, 0] = high
    ref[index, 1] = low


def prep_top(small_ref, where_ref, top_ref):
    zh = where_ref[1]
    total = hdot(hdot(small_ref[3], small_ref[2]), hdot(small_ref[1], small_ref[0]))
    row, col = iotas((TOP, 8 * XY))
    in_pick = jnp.where(row == 2 * (col // 8) + zh, 1.0, 0.0)
    wide = hdot(total[:, :TOP], in_pick)
    row, col = iotas((8 * XY, 8 * XY))
    same = jnp.where(row % 8 == col % 8, 1.0, 0.0)
    row, col = iotas((8 * XY, TOP))
    for index in range(2):
        pick = jnp.where(col == 2 * (row // 8) + (zh if index == 0 else 1 - zh), 1.0, 0.0)
        put(
            top_ref,
            index,
            jnp.concatenate([hdot(pick, wide[:TOP]) * same, hdot(pick, wide[TOP:]) * same], axis=1),
        )


def three_passes(matrices):
    columns = 3 * TOP * len(matrices)
    row, col = iotas((TOP, columns))
    wide = sum(
        hdot(matrix[:, :TOP], jnp.where((col % TOP == row) & (col // (3 * TOP) == index), 1.0, 0.0))
        for index, matrix in enumerate(matrices)
    )
    high = wide.astype(BF16).astype(F32)
    _, col = iotas(wide.shape)
    return jnp.where(col // TOP % 3 == 1, wide - high, high).astype(BF16)


def spread_mid(matrix):
    row, col = iotas((MID, 4 * MID))
    wide = hdot(matrix[:, :MID], jnp.where(row == col % MID, 1.0, 0.0))
    row, col = iotas((4 * MID, MID))
    pick = jnp.where(col == row % MID, 1.0, 0.0)
    row, col = iotas((4 * MID, 4 * MID))
    same = jnp.where(row // MID == col // MID, 1.0, 0.0)
    return jnp.concatenate([hdot(pick, wide[:MID]) * same, hdot(pick, wide[MID:]) * same], axis=1)


def prep_block(refs, block, slot, mid, low):
    small_ref, large_ref, masks_ref, where_ref, built_ref = refs
    flip, phase = masks_ref[block], masks_ref[BLOCKS + block]
    source = where_ref[0] if block == 1 else jnp.bitwise_xor(where_ref[0], where_ref[2])
    scale = sign_of(jnp.bitwise_and(source, masks_ref[2 * BLOCKS + block]))
    fold = fold_left(2 * MID, flip // LOW % MID, phase // LOW % MID)
    full = fold_right(2 * LOW, flip % LOW, phase % LOW)
    put_pair(built_ref, slot, hdot(fold, hdot(small_ref[13 + block], mid)), hdot(hdot(low, large_ref[3 + block]), full))
    fold = fold_left(2 * TOP, flip // (MID * LOW), phase // (MID * LOW))
    return hdot(fold, hdot(small_ref[8 + 2 * block], small_ref[7 + 2 * block])) * scale


def put_pair(ref, slot, mid, low):
    put(ref.at[:, :, : 4 * MID], slot, spread_mid(mid))
    put(ref.at[:, :, 4 * MID :], slot, jnp.concatenate([low, times_i(low)], axis=1))


def merged(small_ref, large_ref):
    mid = hdot(hdot(small_ref[6], small_ref[5]), small_ref[4])
    return mid, hdot(hdot(large_ref[0], large_ref[1]), large_ref[2])


def parts_of(ref, slot):
    pair = ref.at[slot]
    return tuple((pair[0, rows], pair[1, rows]) for rows in (slice(0, 4 * MID), slice(4 * MID, 8 * MID)))


def prep_send(small_ref, large_ref, masks_ref, where_ref, high_ref, built_ref):
    refs = (small_ref, large_ref, masks_ref, where_ref, built_ref)
    mid, low = merged(small_ref, large_ref)
    high_ref[...] = three_passes([prep_block(refs, slot + 1, slot, mid, low) for slot in range(2)])


def prep_keep(small_ref, large_ref, masks_ref, where_ref, high_ref, built_ref):
    refs = (small_ref, large_ref, masks_ref, where_ref, built_ref)
    mid, low = merged(small_ref, large_ref)
    high_ref[...] = three_passes([prep_block(refs, 0, 0, mid, low)])
    put_pair(built_ref, 1, mid, low)


def two_streams(out_ref, first, value):
    half = XY // 2
    out_ref[:, first] = value
    out_ref[:half, first + 1] = value[half:]
    out_ref[half:, first + 1] = value[:half]


def top_kernel(field_ref, top_ref, own_ref, other_ref, early_ref):
    for rest in range(2):
        for pair in range(2):
            parts = [
                field_ref[:, rest, 16 * pair + 8 * half : 16 * pair + 8 * half + 8, :].reshape(8 * XY, 2 * LOW)
                for half in range(2)
            ]
            right = jnp.concatenate(
                [jnp.concatenate(parts, axis=1), jnp.concatenate([times_i(part) for part in parts], axis=1)], axis=0
            )
            right = split(right)
            for index, out_ref in enumerate((own_ref, other_ref)):
                done = dot3((top_ref[index, 0], top_ref[index, 1]), right)
                for half in range(2):
                    group = 2 * pair + half
                    value = done[:, 2 * LOW * half : 2 * LOW * (half + 1)].reshape(XY, 8, 2 * LOW)
                    if group == 0:
                        two_streams(early_ref.at[:, :, rest], 2 * index, value)
                    else:
                        out_ref[:, rest, 8 * group - EARLY : 8 * group - EARLY + 8, :] = value


def add_kernel(own_ref, got_ref, out_ref):
    two_streams(out_ref, 0, own_ref[...] + got_ref[...])


def low_mid(load, mid, low, store):
    for group in range(4):
        done = dot3(split(load(group)), low)
        same, turned = done[:, : 2 * LOW], done[:, 2 * LOW :]
        right = jnp.concatenate(
            [
                jnp.concatenate([same[: 4 * MID], same[4 * MID :]], axis=1),
                jnp.concatenate([turned[: 4 * MID], turned[4 * MID :]], axis=1),
            ],
            axis=0,
        )
        done = dot3(mid, split(right))
        store(group, jnp.concatenate([done[:, : 2 * LOW], done[:, 2 * LOW :]], axis=0))


def high_step(sources, matrix_ref, out_ref):
    matrix = matrix_ref[...]
    for item in range(0, MID, 2):
        right = []
        for source_ref in sources:
            parts = [source_ref[pl.ds(item + half, TOP, stride=MID), :] for half in range(2)]
            high, low = split(jnp.concatenate(parts, axis=1))
            right += [high, high, low]
        total = jnp.dot(matrix, jnp.concatenate(right, axis=0), preferred_element_type=F32)
        for half in range(2):
            part = total[:, 2 * LOW * half : 2 * LOW * (half + 1)]
            out_ref[pl.ds(item + half, TOP, stride=MID), :] = part[:TOP] + times_i(part[TOP:])


def reader(fields, stream):
    early_ref, got_ref, late_ref = fields

    def load(group):
        part = slice(4 * group, 4 * group + 4)
        early = early_ref[part, stream] + got_ref[part, stream]
        return jnp.concatenate(
            [early.reshape(8, EARLY, 2 * LOW), late_ref[part, stream].reshape(8, MID - EARLY, 2 * LOW)], axis=1
        ).reshape(8 * MID, 2 * LOW)

    return load


def writer(ref):
    def store(group, value):
        ref[8 * MID * group : 8 * MID * (group + 1)] = value

    return store


def send_kernel(early_ref, got_ref, late_ref, high_ref, built_ref, out_ref, first_ref, second_ref):
    fields = (early_ref, got_ref, late_ref)
    for slot, half_ref in enumerate((first_ref, second_ref)):
        mid, low = parts_of(built_ref, slot)
        low_mid(reader(fields, slot), mid, low, writer(half_ref))
    high_step((first_ref, second_ref), high_ref, out_ref)


def keep_kernel(early_ref, got_ref, late_ref, high_ref, built_ref, final_ref, out_ref, first_ref):
    fields = (early_ref, got_ref, late_ref)
    mid, low = parts_of(built_ref, 0)
    low_mid(reader(fields, 1), mid, low, writer(first_ref))
    high_step((first_ref,), high_ref, out_ref)
    mid, low = parts_of(built_ref, 1)
    low_mid(reader(fields, 0), mid, low, writer(final_ref))


def real_form(matrix):
    real, imag = matrix[:, 0], matrix[:, 1]
    return jnp.concatenate(
        [jnp.concatenate([real, -imag], axis=2), jnp.concatenate([imag, real], axis=2)], axis=1
    )


def flat_form(matrix):
    real, imag = jnp.swapaxes(matrix[:, 0], 1, 2), jnp.swapaxes(matrix[:, 1], 1, 2)
    return jnp.concatenate(
        [jnp.concatenate([real, imag], axis=2), jnp.concatenate([-imag, real], axis=2)], axis=1
    )


def vm():
    return pl.BlockSpec(memory_space=pltpu.VMEM)


def sm():
    return pl.BlockSpec(memory_space=pltpu.SMEM)


def call(body, ins, outs, scratch=(), smem=()):
    return pl.pallas_call(
        body,
        in_specs=[sm() if i in smem else vm() for i in range(ins)],
        out_specs=[vm() for _ in outs],
        out_shape=[jax.ShapeDtypeStruct(s, t) for s, t in outs],
        scratch_shapes=[pltpu.VMEM(s, t) for s, t in scratch],
        compiler_params=pltpu.CompilerParams(vmem_limit_bytes=16 * 2**20),
    )


def evolve(
    amplitudes,
    top_gates,
    mid_gates,
    low_gates,
    ham_top,
    ham_mid,
    ham_low,
    flip_masks,
    phase_masks,
    device_phase_masks,
):
    width = 2 * LOW
    inside = lax.all_to_all(
        amplitudes.reshape(XY, 2 * MID, width), ("x", "y"), split_axis=0, concat_axis=0, tiled=True
    ).reshape(XY, 2, MID, width)
    small = real_form(
        jnp.concatenate([top_gates, mid_gates, ham_top.reshape(2 * BLOCKS, 2, TOP, TOP), ham_mid], axis=0)
    )
    large = flat_form(jnp.concatenate([low_gates, ham_low], axis=0))
    zh = lax.axis_index("zh")
    n = lax.axis_index("narrow")
    device_id = ((lax.axis_index("x") * 4 + lax.axis_index("y")) * 2 + zh) * 8 + n
    where = jnp.stack([device_id, zh, jnp.int32(16 * 8)]).astype(jnp.int32)
    masks = jnp.concatenate([flip_masks, phase_masks, device_phase_masks])
    (top,) = call(prep_top, 2, [((2, 2, 128, 256), BF16)], smem=(1,))(small, where)
    late = MID - EARLY
    piece = ((XY, 2, late, width), F32)
    own, other, early = call(top_kernel, 2, [piece, piece, ((XY, 4, 2, EARLY, width), F32)])(inside, top)
    swap = [(0, 1), (1, 0)]
    got = lax.ppermute(other, "zh", swap)
    early = lax.all_to_all(
        early.reshape(XY, 8 * EARLY, width), ("x", "y"), split_axis=0, concat_axis=0, tiled=True
    ).reshape(XY, 4, 2, EARLY, width)
    early_got = lax.ppermute(early[:, 2:], "zh", swap)
    (both,) = call(add_kernel, 2, [((XY, 2, 2, late, width), F32)])(own, got)
    field = lax.all_to_all(
        both.reshape(XY, 4 * late, width), ("x", "y"), split_axis=0, concat_axis=0, tiled=True
    ).reshape(XY, 2, 2, late, width)
    built = ((2, 2, 8 * MID, 256), BF16)
    prepared = call(prep_send, 4, [((2 * TOP, 6 * TOP), BF16), built], smem=(2, 3))(small, large, masks, where)
    whole = ((TOP * MID, width), F32)
    fields = (early, early_got, field)
    (sent,) = call(send_kernel, 5, [whole], [whole, whole])(*fields, *prepared)
    arrived = lax.ppermute(sent, "narrow", [(i, i ^ 4) for i in range(8)])
    prepared = call(prep_keep, 4, [((2 * TOP, 3 * TOP), BF16), built], smem=(2, 3))(small, large, masks, where)
    final, kept = call(keep_kernel, 5, [whole, whole], [whole])(*fields, *prepared)
    return final, kept + arrived


def solution(mesh):
    fine = Mesh(mesh.devices.reshape(4, 4, 2, 8), ("x", "y", "zh", "narrow"))
    rows = P(("x", "y", "zh", "narrow"), None)
    return jax.shard_map(
        evolve,
        mesh=fine,
        in_specs=(rows, P(), P(), P(), P(), P(), P(), P(), P(), P()),
        out_specs=(rows, rows),
        check_vma=False,
    )
```

```python
import jax
import jax.numpy as jnp
from jax import lax
from jax.experimental import pallas as pl
from jax.experimental.pallas import tpu as pltpu
from jax.sharding import Mesh, PartitionSpec as P


TOP = 32
MID = 32
LOW = 64
BLOCKS = 3
XY = 16
EARLY = 8
HIGH = lax.Precision.HIGHEST
F32 = jnp.float32
BF16 = jnp.bfloat16


def split(value):
    high = value.astype(BF16)
    return high, (value - high.astype(F32)).astype(BF16)


def dot3(left, right):
    high, low = left
    upper, lower = right
    return jnp.dot(
        jnp.concatenate([high, low, high], axis=1),
        jnp.concatenate([upper, upper, lower], axis=0),
        preferred_element_type=F32,
    )


def times_i(value):
    lane = lax.broadcasted_iota(jnp.int32, value.shape, 1)
    turned = pltpu.roll(value, LOW, 1)
    return jnp.where(lane < LOW, -turned, turned)


def iotas(shape):
    return lax.broadcasted_iota(jnp.int32, shape, 0), lax.broadcasted_iota(jnp.int32, shape, 1)


def sign_of(bits):
    for offset in (8, 4, 2, 1):
        bits = jnp.bitwise_xor(bits, jnp.right_shift(bits, offset))
    return (1 - 2 * jnp.bitwise_and(bits, 1)).astype(F32)


def hdot(left, right):
    return jnp.dot(left, right, precision=HIGH, preferred_element_type=F32)


def fold_left(order, flip, phase):
    row, col = iotas((order, order))
    return jnp.where(col == jnp.bitwise_xor(row, flip), sign_of(jnp.bitwise_and(col, phase)), 0.0)


def fold_right(order, flip, phase):
    row, col = iotas((order, order))
    return jnp.where(row == jnp.bitwise_xor(col, flip), sign_of(jnp.bitwise_and(row, phase)), 0.0)


def put(ref, index, value):
    high, low = split(value)
    ref[index, 0] = high
    ref[index, 1] = low


def prep_top(small_ref, where_ref, top_ref):
    zh = where_ref[1]
    total = hdot(hdot(small_ref[3], small_ref[2]), hdot(small_ref[1], small_ref[0]))
    row, col = iotas((TOP, 8 * XY))
    in_pick = jnp.where(row == 2 * (col // 8) + zh, 1.0, 0.0)
    wide = hdot(total[:, :TOP], in_pick)
    row, col = iotas((8 * XY, 8 * XY))
    same = jnp.where(row % 8 == col % 8, 1.0, 0.0)
    row, col = iotas((8 * XY, TOP))
    for index in range(2):
        pick = jnp.where(col == 2 * (row // 8) + (zh if index == 0 else 1 - zh), 1.0, 0.0)
        put(
            top_ref,
            index,
            jnp.concatenate([hdot(pick, wide[:TOP]) * same, hdot(pick, wide[TOP:]) * same], axis=1),
        )


def three_passes(matrices):
    columns = 3 * TOP * len(matrices)
    row, col = iotas((TOP, columns))
    wide = sum(
        hdot(matrix[:, :TOP], jnp.where((col % TOP == row) & (col // (3 * TOP) == index), 1.0, 0.0))
        for index, matrix in enumerate(matrices)
    )
    high = wide.astype(BF16).astype(F32)
    _, col = iotas(wide.shape)
    return jnp.where(col // TOP % 3 == 1, wide - high, high).astype(BF16)


def prep_block(refs, block, slot, mid, low):
    small_ref, large_ref, masks_ref, where_ref, mid_ref, low_ref = refs
    flip, phase = masks_ref[block], masks_ref[BLOCKS + block]
    source = where_ref[0] if block == 1 else jnp.bitwise_xor(where_ref[0], where_ref[2])
    scale = sign_of(jnp.bitwise_and(source, masks_ref[2 * BLOCKS + block]))
    fold = fold_left(2 * MID, flip // LOW % MID, phase // LOW % MID)
    full = fold_right(2 * LOW, flip % LOW, phase % LOW)
    mid_ref[slot] = three_passes([hdot(fold, hdot(small_ref[13 + block], mid))])
    put(low_ref, slot, hdot(hdot(low, large_ref[3 + block]), full))
    fold = fold_left(2 * TOP, flip // (MID * LOW), phase // (MID * LOW))
    return hdot(fold, hdot(small_ref[8 + 2 * block], small_ref[7 + 2 * block])) * scale


def merged(small_ref, large_ref):
    mid = hdot(hdot(small_ref[6], small_ref[5]), small_ref[4])
    return mid, hdot(hdot(large_ref[0], large_ref[1]), large_ref[2])


def prep_send(*refs):
    mid, low = merged(*refs[:2])
    refs[6][...] = three_passes([prep_block(refs[:6], slot + 1, slot, mid, low) for slot in range(2)])


def prep_keep(*refs):
    mid, low = merged(*refs[:2])
    refs[6][...] = three_passes([prep_block(refs[:6], 0, 0, mid, low)])
    refs[4][1] = three_passes([mid])
    put(refs[5], 1, low)


def two_streams(out_ref, first, value):
    half = XY // 2
    out_ref[:, first] = value
    out_ref[:half, first + 1] = value[half:]
    out_ref[half:, first + 1] = value[:half]


def top_kernel(field_ref, top_ref, own_ref, other_ref, early_ref):
    for rest in range(2):
        for pair in range(2):
            parts = [
                field_ref[:, rest, 16 * pair + 8 * half : 16 * pair + 8 * half + 8, :].reshape(8 * XY, 2 * LOW)
                for half in range(2)
            ]
            right = jnp.concatenate(
                [jnp.concatenate(parts, axis=1), jnp.concatenate([times_i(part) for part in parts], axis=1)], axis=0
            )
            right = split(right)
            for index, out_ref in enumerate((own_ref, other_ref)):
                done = dot3((top_ref[index, 0], top_ref[index, 1]), right)
                for half in range(2):
                    group = 2 * pair + half
                    value = done[:, 2 * LOW * half : 2 * LOW * (half + 1)].reshape(XY, 8, 2 * LOW)
                    if group == 0:
                        two_streams(early_ref.at[:, :, rest], 2 * index, value)
                    else:
                        out_ref[:, rest, 8 * group - EARLY : 8 * group - EARLY + 8, :] = value


def add_kernel(own_ref, got_ref, out_ref):
    two_streams(out_ref, 0, own_ref[...] + got_ref[...])


def low_mid(load, mid, low, store):
    for group in range(4):
        high, rest = split(dot3(split(load(group)), low))
        values = []
        for pair in range(4):
            parts = [
                jnp.concatenate([part[2 * MID * pair : 2 * MID * pair + MID], part[2 * MID * pair + MID : 2 * MID * (pair + 1)]], axis=1)
                for part in (high, rest)
            ]
            total = jnp.dot(
                mid, jnp.concatenate([parts[0], parts[0], parts[1]], axis=0), preferred_element_type=F32
            )
            for half in range(2):
                part = total[:, 2 * LOW * half : 2 * LOW * (half + 1)]
                values.append(part[:MID] + times_i(part[MID:]))
        store(group, jnp.concatenate(values, axis=0))


def high_step(sources, matrix_ref, out_ref):
    matrix = matrix_ref[...]
    for item in range(0, MID, 2):
        right = []
        for source_ref in sources:
            parts = [source_ref[pl.ds(item + half, TOP, stride=MID), :] for half in range(2)]
            high, low = split(jnp.concatenate(parts, axis=1))
            right += [high, high, low]
        total = jnp.dot(matrix, jnp.concatenate(right, axis=0), preferred_element_type=F32)
        for half in range(2):
            part = total[:, 2 * LOW * half : 2 * LOW * (half + 1)]
            out_ref[pl.ds(item + half, TOP, stride=MID), :] = part[:TOP] + times_i(part[TOP:])


def reader(fields, stream):
    early_ref, got_ref, late_ref = fields

    def load(group):
        part = slice(4 * group, 4 * group + 4)
        early = early_ref[part, stream] + got_ref[part, stream]
        return jnp.concatenate(
            [early.reshape(8, EARLY, 2 * LOW), late_ref[part, stream].reshape(8, MID - EARLY, 2 * LOW)], axis=1
        ).reshape(8 * MID, 2 * LOW)

    return load


def writer(ref):
    def store(group, value):
        ref[8 * MID * group : 8 * MID * (group + 1)] = value

    return store


def low_of(ref, slot):
    return ref[slot, 0], ref[slot, 1]


def send_kernel(early_ref, got_ref, late_ref, mid_ref, low_ref, high_ref, out_ref, first_ref, second_ref):
    fields = (early_ref, got_ref, late_ref)
    for slot, half_ref in enumerate((first_ref, second_ref)):
        low_mid(reader(fields, slot), mid_ref[slot], low_of(low_ref, slot), writer(half_ref))
    high_step((first_ref, second_ref), high_ref, out_ref)


def keep_kernel(early_ref, got_ref, late_ref, mid_ref, low_ref, high_ref, final_ref, out_ref, first_ref):
    fields = (early_ref, got_ref, late_ref)
    low_mid(reader(fields, 1), mid_ref[0], low_of(low_ref, 0), writer(first_ref))
    high_step((first_ref,), high_ref, out_ref)
    low_mid(reader(fields, 0), mid_ref[1], low_of(low_ref, 1), writer(final_ref))


def real_form(matrix):
    real, imag = matrix[:, 0], matrix[:, 1]
    return jnp.concatenate(
        [jnp.concatenate([real, -imag], axis=2), jnp.concatenate([imag, real], axis=2)], axis=1
    )


def flat_form(matrix):
    real, imag = jnp.swapaxes(matrix[:, 0], 1, 2), jnp.swapaxes(matrix[:, 1], 1, 2)
    return jnp.concatenate(
        [jnp.concatenate([real, imag], axis=2), jnp.concatenate([-imag, real], axis=2)], axis=1
    )


def vm():
    return pl.BlockSpec(memory_space=pltpu.VMEM)


def sm():
    return pl.BlockSpec(memory_space=pltpu.SMEM)


def call(body, ins, outs, scratch=(), smem=()):
    return pl.pallas_call(
        body,
        in_specs=[sm() if i in smem else vm() for i in range(ins)],
        out_specs=[vm() for _ in outs],
        out_shape=[jax.ShapeDtypeStruct(s, t) for s, t in outs],
        scratch_shapes=[pltpu.VMEM(s, t) for s, t in scratch],
        compiler_params=pltpu.CompilerParams(vmem_limit_bytes=16 * 2**20),
    )


def evolve(
    amplitudes,
    top_gates,
    mid_gates,
    low_gates,
    ham_top,
    ham_mid,
    ham_low,
    flip_masks,
    phase_masks,
    device_phase_masks,
):
    width = 2 * LOW
    inside = lax.all_to_all(
        amplitudes.reshape(XY, 2 * MID, width), ("x", "y"), split_axis=0, concat_axis=0, tiled=True
    ).reshape(XY, 2, MID, width)
    small = real_form(
        jnp.concatenate([top_gates, mid_gates, ham_top.reshape(2 * BLOCKS, 2, TOP, TOP), ham_mid], axis=0)
    )
    large = flat_form(jnp.concatenate([low_gates, ham_low], axis=0))
    zh = lax.axis_index("zh")
    n = lax.axis_index("narrow")
    device_id = ((lax.axis_index("x") * 4 + lax.axis_index("y")) * 2 + zh) * 8 + n
    where = jnp.stack([device_id, zh, jnp.int32(16 * 8)]).astype(jnp.int32)
    masks = jnp.concatenate([flip_masks, phase_masks, device_phase_masks])
    (top,) = call(prep_top, 2, [((2, 2, 128, 256), BF16)], smem=(1,))(small, where)
    late = MID - EARLY
    piece = ((XY, 2, late, width), F32)
    own, other, early = call(top_kernel, 2, [piece, piece, ((XY, 4, 2, EARLY, width), F32)])(inside, top)
    swap = [(0, 1), (1, 0)]
    got = lax.ppermute(other, "zh", swap)
    early = lax.all_to_all(
        early.reshape(XY, 8 * EARLY, width), ("x", "y"), split_axis=0, concat_axis=0, tiled=True
    ).reshape(XY, 4, 2, EARLY, width)
    early_got = lax.ppermute(early[:, 2:], "zh", swap)
    (both,) = call(add_kernel, 2, [((XY, 2, 2, late, width), F32)])(own, got)
    field = lax.all_to_all(
        both.reshape(XY, 4 * late, width), ("x", "y"), split_axis=0, concat_axis=0, tiled=True
    ).reshape(XY, 2, 2, late, width)
    built = [((2, 2 * MID, 3 * MID), BF16), ((2, 2, width, width), BF16)]
    prepared = call(prep_send, 4, built + [((2 * TOP, 6 * TOP), BF16)], smem=(2, 3))(small, large, masks, where)
    whole = ((TOP * MID, width), F32)
    fields = (early, early_got, field)
    (sent,) = call(send_kernel, 6, [whole], [whole, whole])(*fields, *prepared)
    arrived = lax.ppermute(sent, "narrow", [(i, i ^ 4) for i in range(8)])
    prepared = call(prep_keep, 4, built + [((2 * TOP, 3 * TOP), BF16)], smem=(2, 3))(small, large, masks, where)
    final, kept = call(keep_kernel, 6, [whole, whole], [whole])(*fields, *prepared)
    return final, kept + arrived


def solution(mesh):
    fine = Mesh(mesh.devices.reshape(4, 4, 2, 8), ("x", "y", "zh", "narrow"))
    rows = P(("x", "y", "zh", "narrow"), None)
    return jax.shard_map(
        evolve,
        mesh=fine,
        in_specs=(rows, P(), P(), P(), P(), P(), P(), P(), P(), P()),
        out_specs=(rows, rows),
        check_vma=False,
    )
```

```python
import jax
import jax.numpy as jnp
from jax import lax
from jax.experimental import pallas as pl
from jax.experimental.pallas import tpu as pltpu
from jax.sharding import Mesh, PartitionSpec as P


TOP = 32
MID = 32
LOW = 64
BLOCKS = 3
XY = 16
EARLY = 8
HIGH = lax.Precision.HIGHEST
F32 = jnp.float32
BF16 = jnp.bfloat16


def split(value):
    high = value.astype(BF16)
    return high, (value - high.astype(F32)).astype(BF16)


def dot3(left, right):
    high, low = left
    upper, lower = right
    return jnp.dot(
        jnp.concatenate([high, low, high], axis=1),
        jnp.concatenate([upper, upper, lower], axis=0),
        preferred_element_type=F32,
    )


def times_i(value):
    lane = lax.broadcasted_iota(jnp.int32, value.shape, 1)
    turned = pltpu.roll(value, LOW, 1)
    return jnp.where(lane < LOW, -turned, turned)


def iotas(shape):
    return lax.broadcasted_iota(jnp.int32, shape, 0), lax.broadcasted_iota(jnp.int32, shape, 1)


def sign_of(bits):
    for offset in (8, 4, 2, 1):
        bits = jnp.bitwise_xor(bits, jnp.right_shift(bits, offset))
    return (1 - 2 * jnp.bitwise_and(bits, 1)).astype(F32)


def hdot(left, right):
    return jnp.dot(left, right, precision=HIGH, preferred_element_type=F32)


def fold_left(order, flip, phase):
    row, col = iotas((order, order))
    return jnp.where(col == jnp.bitwise_xor(row, flip), sign_of(jnp.bitwise_and(col, phase)), 0.0)


def fold_right(order, flip, phase):
    row, col = iotas((order, order))
    return jnp.where(row == jnp.bitwise_xor(col, flip), sign_of(jnp.bitwise_and(row, phase)), 0.0)


def put(ref, index, value):
    high, low = split(value)
    ref[index, 0] = high
    ref[index, 1] = low


def prep_top(small_ref, where_ref, top_ref):
    zh = where_ref[1]
    total = hdot(hdot(small_ref[3], small_ref[2]), hdot(small_ref[1], small_ref[0]))
    row, col = iotas((TOP, 8 * XY))
    in_pick = jnp.where(row == 2 * (col // 8) + zh, 1.0, 0.0)
    wide = hdot(total[:, :TOP], in_pick)
    row, col = iotas((8 * XY, 8 * XY))
    same = jnp.where(row % 8 == col % 8, 1.0, 0.0)
    row, col = iotas((8 * XY, TOP))
    for index in range(2):
        pick = jnp.where(col == 2 * (row // 8) + (zh if index == 0 else 1 - zh), 1.0, 0.0)
        put(
            top_ref,
            index,
            jnp.concatenate([hdot(pick, wide[:TOP]) * same, hdot(pick, wide[TOP:]) * same], axis=1),
        )


def three_passes(matrices):
    columns = 3 * TOP * len(matrices)
    row, col = iotas((TOP, columns))
    wide = sum(
        hdot(matrix[:, :TOP], jnp.where((col % TOP == row) & (col // (3 * TOP) == index), 1.0, 0.0))
        for index, matrix in enumerate(matrices)
    )
    high = wide.astype(BF16).astype(F32)
    _, col = iotas(wide.shape)
    return jnp.where(col // TOP % 3 == 1, wide - high, high).astype(BF16)


def prep_block(refs, block, slot, mid, low):
    small_ref, large_ref, masks_ref, where_ref, mid_ref, low_ref = refs
    flip, phase = masks_ref[block], masks_ref[BLOCKS + block]
    source = where_ref[0] if block == 1 else jnp.bitwise_xor(where_ref[0], where_ref[2])
    scale = sign_of(jnp.bitwise_and(source, masks_ref[2 * BLOCKS + block]))
    fold = fold_left(2 * MID, flip // LOW % MID, phase // LOW % MID)
    full = fold_right(2 * LOW, flip % LOW, phase % LOW)
    mid_ref[slot] = three_passes([hdot(fold, hdot(small_ref[13 + block], mid))])
    put(low_ref, slot, hdot(hdot(low, large_ref[3 + block]), full))
    fold = fold_left(2 * TOP, flip // (MID * LOW), phase // (MID * LOW))
    return hdot(fold, hdot(small_ref[8 + 2 * block], small_ref[7 + 2 * block])) * scale


def merged(small_ref, large_ref):
    mid = hdot(hdot(small_ref[6], small_ref[5]), small_ref[4])
    return mid, hdot(hdot(large_ref[0], large_ref[1]), large_ref[2])


def prep_send(*refs):
    mid, low = merged(*refs[:2])
    refs[6][...] = three_passes([prep_block(refs[:6], slot + 1, slot, mid, low) for slot in range(2)])


def prep_keep(*refs):
    mid, low = merged(*refs[:2])
    refs[6][...] = three_passes([prep_block(refs[:6], 0, 0, mid, low)])
    refs[4][1] = three_passes([mid])
    put(refs[5], 1, low)


def two_streams(out_ref, first, value):
    half = XY // 2
    out_ref[:, first] = value
    out_ref[:half, first + 1] = value[half:]
    out_ref[half:, first + 1] = value[:half]


def top_kernel(field_ref, top_ref, own_ref, other_ref, early_ref):
    for rest in range(2):
        for pair in range(2):
            parts = [
                field_ref[:, rest, 16 * pair + 8 * half : 16 * pair + 8 * half + 8, :].reshape(8 * XY, 2 * LOW)
                for half in range(2)
            ]
            right = jnp.concatenate(
                [jnp.concatenate(parts, axis=1), jnp.concatenate([times_i(part) for part in parts], axis=1)], axis=0
            )
            right = split(right)
            for index, out_ref in enumerate((own_ref, other_ref)):
                done = dot3((top_ref[index, 0], top_ref[index, 1]), right)
                for half in range(2):
                    group = 2 * pair + half
                    value = done[:, 2 * LOW * half : 2 * LOW * (half + 1)].reshape(XY, 8, 2 * LOW)
                    if group == 0:
                        two_streams(early_ref.at[:, :, rest], 2 * index, value)
                    else:
                        out_ref[:, rest, 8 * group - EARLY : 8 * group - EARLY + 8, :] = value


def add_kernel(own_ref, got_ref, out_ref):
    two_streams(out_ref, 0, own_ref[...] + got_ref[...])


def low_mid(load, mid, low, store):
    for group in range(4):
        high, rest = split(dot3(split(load(group)), low))
        values = []
        for pair in range(4):
            parts = [
                jnp.concatenate([part[2 * MID * pair : 2 * MID * pair + MID], part[2 * MID * pair + MID : 2 * MID * (pair + 1)]], axis=1)
                for part in (high, rest)
            ]
            total = jnp.dot(
                mid, jnp.concatenate([parts[0], parts[0], parts[1]], axis=0), preferred_element_type=F32
            )
            for half in range(2):
                part = total[:, 2 * LOW * half : 2 * LOW * (half + 1)]
                values.append(part[:MID] + times_i(part[MID:]))
        store(group, jnp.concatenate(values, axis=0))


def high_step(sources, matrix_ref, out_ref, first=0, items=MID):
    matrix = matrix_ref[...]
    for item in range(0, items, 2):
        right = []
        for source_ref in sources:
            parts = [source_ref[pl.ds(first + item + half, TOP, stride=MID), :] for half in range(2)]
            high, low = split(jnp.concatenate(parts, axis=1))
            right += [high, high, low]
        total = jnp.dot(matrix, jnp.concatenate(right, axis=0), preferred_element_type=F32)
        for half in range(2):
            part = total[:, 2 * LOW * half : 2 * LOW * (half + 1)]
            out_ref[pl.ds(item + half, TOP, stride=items), :] = part[:TOP] + times_i(part[TOP:])


def reader(fields, stream):
    early_ref, got_ref, late_ref = fields

    def load(group):
        part = slice(4 * group, 4 * group + 4)
        early = early_ref[part, stream] + got_ref[part, stream]
        return jnp.concatenate(
            [early.reshape(8, EARLY, 2 * LOW), late_ref[part, stream].reshape(8, MID - EARLY, 2 * LOW)], axis=1
        ).reshape(8 * MID, 2 * LOW)

    return load


def writer(ref):
    def store(group, value):
        ref[8 * MID * group : 8 * MID * (group + 1)] = value

    return store


def low_of(ref, slot):
    return ref[slot, 0], ref[slot, 1]


def send_kernel(early_ref, got_ref, late_ref, mid_ref, low_ref, high_ref, out_ref, first_ref, second_ref):
    fields = (early_ref, got_ref, late_ref)
    for slot, half_ref in enumerate((first_ref, second_ref)):
        low_mid(reader(fields, slot), mid_ref[slot], low_of(low_ref, slot), writer(half_ref))
    high_step((first_ref, second_ref), high_ref, out_ref, 0, MID // 2)


def rest_kernel(first_ref, second_ref, high_ref, out_ref):
    high_step((first_ref, second_ref), high_ref, out_ref, MID // 2, MID // 2)


def keep_kernel(early_ref, got_ref, late_ref, mid_ref, low_ref, high_ref, final_ref, out_ref, first_ref):
    fields = (early_ref, got_ref, late_ref)
    low_mid(reader(fields, 1), mid_ref[0], low_of(low_ref, 0), writer(first_ref))
    high_step((first_ref,), high_ref, out_ref)
    low_mid(reader(fields, 0), mid_ref[1], low_of(low_ref, 1), writer(final_ref))


def real_form(matrix):
    real, imag = matrix[:, 0], matrix[:, 1]
    return jnp.concatenate(
        [jnp.concatenate([real, -imag], axis=2), jnp.concatenate([imag, real], axis=2)], axis=1
    )


def flat_form(matrix):
    real, imag = jnp.swapaxes(matrix[:, 0], 1, 2), jnp.swapaxes(matrix[:, 1], 1, 2)
    return jnp.concatenate(
        [jnp.concatenate([real, imag], axis=2), jnp.concatenate([-imag, real], axis=2)], axis=1
    )


def vm():
    return pl.BlockSpec(memory_space=pltpu.VMEM)


def sm():
    return pl.BlockSpec(memory_space=pltpu.SMEM)


def call(body, ins, outs, scratch=(), smem=()):
    return pl.pallas_call(
        body,
        in_specs=[sm() if i in smem else vm() for i in range(ins)],
        out_specs=[vm() for _ in outs],
        out_shape=[jax.ShapeDtypeStruct(s, t) for s, t in outs],
        scratch_shapes=[pltpu.VMEM(s, t) for s, t in scratch],
        compiler_params=pltpu.CompilerParams(vmem_limit_bytes=16 * 2**20),
    )


def evolve(
    amplitudes,
    top_gates,
    mid_gates,
    low_gates,
    ham_top,
    ham_mid,
    ham_low,
    flip_masks,
    phase_masks,
    device_phase_masks,
):
    width = 2 * LOW
    inside = lax.all_to_all(
        amplitudes.reshape(XY, 2 * MID, width), ("x", "y"), split_axis=0, concat_axis=0, tiled=True
    ).reshape(XY, 2, MID, width)
    small = real_form(
        jnp.concatenate([top_gates, mid_gates, ham_top.reshape(2 * BLOCKS, 2, TOP, TOP), ham_mid], axis=0)
    )
    large = flat_form(jnp.concatenate([low_gates, ham_low], axis=0))
    zh = lax.axis_index("zh")
    n = lax.axis_index("narrow")
    device_id = ((lax.axis_index("x") * 4 + lax.axis_index("y")) * 2 + zh) * 8 + n
    where = jnp.stack([device_id, zh, jnp.int32(16 * 8)]).astype(jnp.int32)
    masks = jnp.concatenate([flip_masks, phase_masks, device_phase_masks])
    (top,) = call(prep_top, 2, [((2, 2, 128, 256), BF16)], smem=(1,))(small, where)
    late = MID - EARLY
    piece = ((XY, 2, late, width), F32)
    own, other, early = call(top_kernel, 2, [piece, piece, ((XY, 4, 2, EARLY, width), F32)])(inside, top)
    swap = [(0, 1), (1, 0)]
    got = lax.ppermute(other, "zh", swap)
    early = lax.all_to_all(
        early.reshape(XY, 8 * EARLY, width), ("x", "y"), split_axis=0, concat_axis=0, tiled=True
    ).reshape(XY, 4, 2, EARLY, width)
    early_got = lax.ppermute(early[:, 2:], "zh", swap)
    (both,) = call(add_kernel, 2, [((XY, 2, 2, late, width), F32)])(own, got)
    field = lax.all_to_all(
        both.reshape(XY, 4 * late, width), ("x", "y"), split_axis=0, concat_axis=0, tiled=True
    ).reshape(XY, 2, 2, late, width)
    built = [((2, 2 * MID, 3 * MID), BF16), ((2, 2, width, width), BF16)]
    prepared = call(prep_send, 4, built + [((2 * TOP, 6 * TOP), BF16)], smem=(2, 3))(small, large, masks, where)
    whole = ((TOP * MID, width), F32)
    fields = (early, early_got, field)
    half = ((TOP * MID // 2, width), F32)
    sent, *middle = call(send_kernel, 6, [half, whole, whole])(*fields, *prepared)
    route = [(i, i ^ 4) for i in range(8)]
    arrived = [lax.ppermute(sent, "narrow", route)]
    (sent,) = call(rest_kernel, 3, [half])(*middle, prepared[2])
    arrived.append(lax.ppermute(sent, "narrow", route))
    prepared = call(prep_keep, 4, built + [((2 * TOP, 3 * TOP), BF16)], smem=(2, 3))(small, large, masks, where)
    final, kept = call(keep_kernel, 6, [whole, whole], [whole])(*fields, *prepared)
    arrived = jnp.concatenate([part.reshape(TOP, MID // 2, width) for part in arrived], axis=1)
    return final, kept + arrived.reshape(TOP * MID, width)


def solution(mesh):
    fine = Mesh(mesh.devices.reshape(4, 4, 2, 8), ("x", "y", "zh", "narrow"))
    rows = P(("x", "y", "zh", "narrow"), None)
    return jax.shard_map(
        evolve,
        mesh=fine,
        in_specs=(rows, P(), P(), P(), P(), P(), P(), P(), P(), P()),
        out_specs=(rows, rows),
        check_vma=False,
    )
```
